32 devices in a mesh: dp: 2 (over x), lat: 4 (over y, core), lon: 4 (over z).
Axes of the slice: x: 2, y: 2, z: 4, core: 2. Of those that a mesh axis runs over, the one named last changes fastest.
Arguments:
- hidden_in: bfloat16 [2, 64, 512, 128], P('dp', 'lat', 'lon'), may hold values from -6 to 6
- conv_weight: bfloat16 [3, 3, 128, 128], replicated, may hold values from -0.1875 to 0.1875
- conv_bias: float32 [128], replicated, may hold values from -3 to 3
- proj_weight: float32 [128], replicated, may hold values from -5 to 5
- ocean_depth: float32 [64, 512], P('lat', 'lon'), may hold values from 0.5 to 2
- sea_mask: int32 [64, 512], P('lat', 'lon'), may hold values 0 or 1
- step_alpha: float32 [6], replicated, may hold values from 0.04 to 0.07
- step_beta: float32 [6], replicated, may hold values from 0.1 to 0.5
- surface_cotangent: float32 [2, 64, 512], P('dp', 'lat', 'lon'), may hold values from -20 to 20
Outputs:
- grad_hidden: bfloat16 [2, 64, 512, 128], P('dp', 'lat', 'lon')
- grad_weight: float32 [128, 3, 3, 128], P(('lat', 'lon'))
- grad_bias: float32 [128], replicated
- grad_proj: float32 [128], replicated
The draws below stay inside these ranges and needn't reach their ends.
All inputs are finite; a program needn't handle non-finite values. No bound on the sum of `sea_mask` on one device may be relied on, other than what follows from the above.
Results may differ from the reference program's by a relative error of at most 0.01.
Values may be sent and summed in bfloat16 or wider, within the bound.
A program may use at most 64 MiB of HBM per device.

```python
import math
import jax
import jax.numpy as jnp
from jax import lax

C = 128
ITERS = 6
BATCH = 2
NLAT = 64
NLON = 512


def draw_surface_cotangent(key, part):
    key_noise, key_offset, key_sign = jax.random.split(jax.random.fold_in(key, 17), 3)
    lat_ramp = 1.0 + 2.0 * jnp.arange(NLAT, dtype=jnp.float32) / max(NLAT - 1, 1)
    offset = jax.random.uniform(key_offset, (BATCH, 1, 1), jnp.float32, 0.8, 1.5)
    sample_sign = jnp.where(jax.random.bernoulli(key_sign, 0.5, (BATCH, 1, 1)), 1.0, -1.0)
    slope_part = sample_sign * offset * lat_ramp[None, :, None]
    noise_part = jnp.clip(jax.random.normal(key_noise, (BATCH, NLAT, NLON), jnp.float32), -4.0, 4.0)
    values = noise_part + slope_part
    return values


def with_ends(values, own_key, low, top_value):
    shape = values.shape
    spot = [jax.random.randint(jax.random.fold_in(own_key, axis), (), 0, shape[axis]) for axis in range(len(shape))]
    values = values.at[tuple(spot)].set(low)
    longest = shape.index(max(shape))
    spot[longest] = (spot[longest] + 1) % shape[longest]
    return values.at[tuple(spot)].set(top_value)


def block_levels(stream_key, dims, pieces, low, top_value):
    loudness, own = 1.0, jax.random.fold_in(stream_key, 6)
    for axis_at, blocks in pieces:
        steps = jnp.exp(jax.random.uniform(jax.random.fold_in(own, axis_at), (blocks,), jnp.float32, low / len(pieces), top_value / len(pieces)))
        loudness = loudness * jnp.repeat(steps, dims[axis_at] // blocks).reshape([-1 if axis == axis_at else 1 for axis in range(len(dims))])
    return loudness


def gaussian(stream_key, extent, deviation, limit, cuts=(), held_as=jnp.bfloat16):
    entries = jax.random.normal(stream_key, extent, jnp.float32) * deviation
    if len(cuts) > 0:
        entries = block_levels(stream_key, extent, cuts, -0.22, 0.18) * entries
    return jnp.clip(entries, min=-limit, max=limit).astype(held_as)


def setup_inputs(seed: int = 0) -> dict:
    splits = jax.random.split(jax.random.key(seed), 10)
    hidden_in = gaussian(splits[0], (BATCH, NLAT, NLON, C), 1.0, 6.0, ((0, 2), (1, 4), (2, 4)))
    conv_weight = gaussian(splits[1], (3, 3, C, C), (9 * C) ** -0.5, 0.1875)
    conv_bias = gaussian(splits[2], (C,), 0.5, 3.0, (), jnp.float32)
    proj_weight = gaussian(splits[3], (C,), 1.0, 5.0, (), jnp.float32)
    ocean_depth = jnp.clip(jnp.exp(math.log(2.0) - 1.3862944 * jax.random.uniform(splits[4], (NLAT, NLON), jnp.float32) ** block_levels(splits[4], (NLAT, NLON), ((0, 4), (1, 4)), -0.2, 0.2)), 0.5, 2.0)
    sea_mask = with_ends((jax.random.randint(splits[5], (NLAT, NLON), 0, 5) < 4).astype(jnp.int32), jax.random.fold_in(splits[5], 1), 0, 1)
    step_alpha = jnp.clip(jnp.exp(jax.random.uniform(splits[6], (ITERS,), jnp.float32, math.log(0.04), math.log(0.07))), 0.04, 0.07)
    step_beta = jnp.clip(jax.random.uniform(splits[7], (ITERS,), jnp.float32, 0.1, 0.5), 0.1, 0.5)
    surface_cotangent = draw_surface_cotangent(jax.random.fold_in(splits[9], 71), 0)
    return {"hidden_in": hidden_in, "conv_weight": conv_weight, "conv_bias": conv_bias, "proj_weight": proj_weight, "ocean_depth": ocean_depth, "sea_mask": sea_mask, "step_alpha": step_alpha, "step_beta": step_beta, "surface_cotangent": surface_cotangent}


helm_coef = 0.5

def extend(values, lat_axis):
    lon_axis = lat_axis + 1
    length = values.shape[lon_axis]
    left_col = lax.slice_in_dim(values, length - 1, length, axis=lon_axis)
    right_col = lax.slice_in_dim(values, 0, 1, axis=lon_axis)
    wrapped = jnp.concatenate([left_col, values, right_col], axis=lon_axis)
    widths = [(0, 0)] * wrapped.ndim
    widths[lat_axis] = (1, 1)
    return jnp.pad(wrapped, widths)

def operate(field_ext, mask_ext, depth_ext):
    rows_in = field_ext.shape[-2] - 2
    cols_in = field_ext.shape[-1] - 2
    center = field_ext[..., 1:-1, 1:-1]
    mask_mid = mask_ext[1:-1, 1:-1]
    depth_mid = depth_ext[1:-1, 1:-1]
    result = helm_coef * center
    for row_off, col_off in ((0, 1), (2, 1), (1, 0), (1, 2)):
        beside = field_ext[..., row_off:row_off + rows_in, col_off:col_off + cols_in]
        mask_near = mask_ext[row_off:row_off + rows_in, col_off:col_off + cols_in]
        depth_near = depth_ext[row_off:row_off + rows_in, col_off:col_off + cols_in]
        weight = mask_near * 0.5 * (depth_mid + depth_near)
        result = result + weight * (center - beside)
    return mask_mid * result

def solve_steps(adjoint_start, mask_ext, depth_ext, step_alpha, step_beta):
    solution = jnp.zeros_like(adjoint_start)
    residual = adjoint_start
    direction = adjoint_start
    for turn_index in range(ITERS):
        solution = solution + step_alpha[turn_index] * direction
        if turn_index + 1 < ITERS:
            applied = operate(extend(direction, 1), mask_ext, depth_ext)
            residual = residual - step_alpha[turn_index] * applied
            direction = residual + step_beta[turn_index] * direction
    return solution

def reference(hidden_in, conv_weight, conv_bias, proj_weight, ocean_depth, sea_mask, step_alpha, step_beta, surface_cotangent):
    mask_float = sea_mask.astype(jnp.float32)
    ocean_count = jnp.sum(mask_float)
    sample_mean = lax.optimization_barrier(jnp.sum(mask_float * surface_cotangent, axis=(1, 2))) / ocean_count
    adjoint_start = mask_float * (surface_cotangent - sample_mean[:, None, None])
    forcing_grad = mask_float * solve_steps(adjoint_start, extend(mask_float, 0), extend(ocean_depth, 0), step_alpha, step_beta)
    grad_scale = 1.0 / math.sqrt(BATCH * NLAT * NLON)
    grad_weight = jnp.zeros((C, 3, 3, C), jnp.float32)
    grad_bias = jnp.zeros((C,), jnp.float32)
    grad_proj = jnp.zeros((C,), jnp.float32)
    outputs = []
    for sample in range(BATCH):
        padded = extend(hidden_in[sample], 0)
        shifted = [padded[row_off:row_off + NLAT, col_off:col_off + NLON, :].reshape(NLAT * NLON, C) for row_off in range(3) for col_off in range(3)]
        preact = conv_bias
        for offset in range(9):
            preact = preact + jnp.dot(shifted[offset], conv_weight[offset // 3, offset % 3], preferred_element_type=jnp.float32)
        sigma = jax.nn.sigmoid(preact)
        active = preact * sigma
        slope_act = sigma * (1.0 + preact * (1.0 - sigma))
        force_col = forcing_grad[sample].reshape(NLAT * NLON)[:, None]
        grad_pre = (force_col * proj_weight * slope_act).astype(jnp.bfloat16)
        grad_proj = grad_proj + lax.optimization_barrier(jnp.sum(active * force_col, axis=0))
        grad_bias = grad_bias + lax.optimization_barrier(jnp.sum(grad_pre.astype(jnp.float32), axis=0))
        blocks = [jnp.dot(shifted[offset].T, grad_pre, preferred_element_type=jnp.float32) for offset in range(9)]
        grad_weight = grad_weight + jnp.stack(blocks, axis=1).reshape(C, 3, 3, C)
        grad_ext = extend(grad_pre.reshape(NLAT, NLON, C), 0)
        backed = jnp.zeros((NLAT * NLON, C), jnp.float32)
        for row_off in range(3):
            for col_off in range(3):
                window = grad_ext[2 - row_off:2 - row_off + NLAT, 2 - col_off:2 - col_off + NLON, :].reshape(NLAT * NLON, C)
                backed = backed + jnp.dot(window, conv_weight[row_off, col_off].T, preferred_element_type=jnp.float32)
        outputs.append(backed.reshape(NLAT, NLON, C).astype(jnp.bfloat16))
    return (jnp.stack(outputs), grad_weight * grad_scale, grad_bias * grad_scale, grad_proj * grad_scale)
```

```python
import functools
import math

import jax
import jax.numpy as jnp
from jax import lax
from jax.experimental import pallas as pl
from jax.experimental.pallas import tpu as pltpu
from jax.sharding import PartitionSpec as P

MESH = pl.DeviceIdType.MESH
F32 = jnp.float32
BF16 = jnp.bfloat16
HALF = 8


def remote(src, dst, send, recv, device):
    return pltpu.make_async_remote_copy(
        src_ref=src, dst_ref=dst, send_sem=send, recv_sem=recv, device_id=device, device_id_type=MESH
    )


def kernel(dims, *refs):
    ndp, nlat, nlon, rows, cols, chan, iters, fast = dims
    (x_ref, w_ref, bias_ref, proj_ref, depth_ref, mask_ref, alpha_ref, beta_ref, ct_ref) = refs[:9]
    gh_ref, gw_ref, sum_ref = refs[9:12]
    (xs, gs, wb, fld, q_in, ebuf, el_in, ec_in, gbuf, gl_in, gc_in, mean_buf, small_buf, small_dp) = refs[12:26]
    (x_send, x_recv, g_send, g_recv, mean_send, mean_recv, small_send, small_recv, sdp_send, sdp_recv) = refs[26:36]
    if fast:
        (g1, r1, s1, r2, b3, r3, s4) = refs[36:43]
        (r1_send, r1_recv, r2_send, r2_recv, r3_send, r3_recv, r4_send, r4_recv) = refs[43:51]
    dp, la, lo = lax.axis_index("dp"), lax.axis_index("lat"), lax.axis_index("lon")
    group = nlat * nlon
    me = la * nlon + lo
    west, east = lax.rem(lo + nlon - 1, nlon), lax.rem(lo + 1, nlon)
    has_n, has_s = la > 0, la < nlat - 1

    def peer(step):
        spot = lax.rem(me + step, group)
        return spot, {"lat": spot // nlon, "lon": lax.rem(spot, nlon)}

    barrier = pltpu.get_barrier_semaphore()
    for step in range(1, group):
        pl.semaphore_signal(barrier, inc=1, device_id=peer(step)[1], device_id_type=MESH)
    for step in range(1, ndp):
        pl.semaphore_signal(barrier, inc=1, device_id={"dp": lax.rem(dp + step, ndp)}, device_id_type=MESH)

    mask = mask_ref[...].astype(F32)
    wet = mask * depth_ref[...]
    start = mask * ct_ref[0]
    fld[0] = wet
    fld[1] = start
    lane = lax.broadcasted_iota(jnp.int32, (rows, cols), 1)
    ebuf[1] = jnp.where(
        lane < 16,
        wet,
        jnp.where(lane < 64, pltpu.roll(start, 16, 1), jnp.where(lane < cols - 16, pltpu.roll(start, cols - 16, 1), wet)),
    )
    mean_buf[me] = jnp.concatenate(
        [jnp.sum(mask, axis=0, keepdims=True), jnp.sum(start, axis=0, keepdims=True)], axis=0
    )
    for row in range(rows):
        ebuf[0, row : row + 1, :] = x_ref[0, row, 0:16, :].astype(F32)[0:1]
        ebuf[2, row : row + 1, :] = x_ref[0, row, cols - 16 : cols, :].astype(F32)[15:16]

    pl.semaphore_wait(barrier, group - 1 + ndp - 1)

    def halo_copies(send, recv, row_pair, q_pair, line_pair, corner):
        north, south = {"lat": la - 1}, {"lat": la + 1}
        out = []
        out.append((has_n, has_s, remote(row_pair[0], row_pair[1], send.at[0], recv.at[0], north)))
        out.append((has_s, has_n, remote(row_pair[2], row_pair[3], send.at[1], recv.at[1], south)))
        for at in range(2):
            out.append((None, None, remote(line_pair[at][0], line_pair[at][1], send.at[2 + at], recv.at[2 + at], {"lon": (west, east)[at]})))
        for at in range(4):
            up = at < 2
            place = {"lat": la - 1 if up else la + 1, "lon": (west, east)[at % 2]}
            guards = (has_n, has_s) if up else (has_s, has_n)
            out.append(guards + (remote(corner[at][0], corner[at][1], send.at[4 + at], recv.at[4 + at], place),))
        if q_pair is not None:
            out.append((has_n, has_s, remote(q_pair[0], q_pair[1], send.at[8], recv.at[8], north)))
            out.append((has_s, has_n, remote(q_pair[2], q_pair[3], send.at[9], recv.at[9], south)))
        return out

    def guarded(guard, action):
        if guard is None:
            action()
        else:
            pl.when(guard)(action)

    def clear(guard, views):
        @pl.when(jnp.logical_not(guard))
        def _():
            for view in views:
                view[...] = jnp.zeros(view.shape, view.dtype)

    x_copies = halo_copies(
        x_send,
        x_recv,
        (x_ref.at[0, 0], xs.at[1, rows + 1], x_ref.at[0, rows - 1], xs.at[1, 0]),
        (fld.at[:, 0:HALF], q_in.at[0], fld.at[:, rows - HALF : rows], q_in.at[1]),
        ((ebuf.at[0:2], el_in.at[0]), (ebuf.at[1:3], el_in.at[1])),
        (
            (ebuf.at[0:2, 0:HALF], ec_in.at[0]),
            (ebuf.at[1:3, 0:HALF], ec_in.at[1]),
            (ebuf.at[0:2, rows - HALF : rows], ec_in.at[2]),
            (ebuf.at[1:3, rows - HALF : rows], ec_in.at[3]),
        ),
    )
    for at in (8, 9, 4, 5, 6, 7, 2, 3, 0, 1):
        guarded(x_copies[at][0], x_copies[at][2].start)
    mean_copies = []
    for step in range(1, group):
        spot, place = peer(step)
        mean_copies.append(remote(mean_buf.at[me], mean_buf.at[me], mean_send.at[step - 1], mean_recv.at[me], place))
        mean_copies[-1].start()
    clear(has_s, (xs.at[1, rows + 1], q_in.at[0], ec_in.at[0], ec_in.at[1]))
    clear(has_n, (xs.at[1, 0], q_in.at[1], ec_in.at[2], ec_in.at[3]))

    for tap in range(9):
        wb[tap * chan : (tap + 1) * chan, :] = w_ref[(8 - tap) * chan : (9 - tap) * chan, :].astype(F32).T.astype(BF16)
    for row in range(rows):
        own = x_ref[0, row]
        wide = own.astype(F32)
        xs[1, row + 1] = own
        xs[0, row + 1] = pltpu.roll(wide, 1, 0).astype(BF16)
        xs[2, row + 1] = pltpu.roll(wide, cols - 1, 0).astype(BF16)

    for at in range(10):
        guarded(x_copies[at][1], x_copies[at][2].wait_recv)

    tile_row = lax.broadcasted_iota(jnp.int32, (16, chan), 0)

    def fix(stack, row, left, right):
        head = stack[0, row, 0:16, :].astype(F32)
        stack[0, row, 0:16, :] = jnp.where(tile_row == 0, left, head).astype(BF16)
        tail = stack[2, row, cols - 16 : cols, :].astype(F32)
        stack[2, row, cols - 16 : cols, :] = jnp.where(tile_row == 15, right, tail).astype(BF16)

    def fix_ends(stack, top, bottom):
        for row, (left, right) in ((0, top), (rows + 1, bottom)):
            wide = stack[1, row].astype(F32)
            stack[0, row] = pltpu.roll(wide, 1, 0).astype(BF16)
            stack[2, row] = pltpu.roll(wide, cols - 1, 0).astype(BF16)
            fix(stack, row, left, right)

    last = HALF - 1
    fix_ends(
        xs,
        (ec_in[3, 1, last : last + 1, :], ec_in[2, 0, last : last + 1, :]),
        (ec_in[1, 1, 0:1, :], ec_in[0, 0, 0:1, :]),
    )
    for row in range(rows):
        fix(xs, row + 1, el_in[1, 1, row : row + 1, :], el_in[0, 0, row : row + 1, :])

    tall = rows + 2 * HALF
    side_lane = lax.broadcasted_iota(jnp.int32, (tall, cols), 1)
    from_west = jnp.concatenate([ec_in[3, 0], el_in[1, 0], ec_in[1, 0]], axis=0)
    from_east = jnp.concatenate([ec_in[2, 1], el_in[0, 1], ec_in[0, 1]], axis=0)
    near = jnp.logical_or(side_lane < iters - 1, side_lane >= cols - (iters - 1))
    wet_side = jnp.where(near, jnp.where(side_lane < 64, from_east, from_west), 0.0)
    start_side = jnp.where(
        near, jnp.where(side_lane < 64, pltpu.roll(from_east, cols - 16, 1), pltpu.roll(from_west, 16, 1)), 0.0
    )
    wet_all = jnp.concatenate([jnp.concatenate([q_in[1, 0], fld[0], q_in[0, 0]], axis=0), wet_side], axis=1)
    start_all = jnp.concatenate([jnp.concatenate([q_in[1, 1], fld[1], q_in[0, 1]], axis=0), start_side], axis=1)
    turns = ((1, 0), (tall - 1, 0), (1, 1), (2 * cols - 1, 1))
    mask_all = jnp.where(wet_all > 0.0, 1.0, 0.0)
    weights = [
        mask_all * pltpu.roll(mask_all, shift, axis) * (0.5 * (wet_all + pltpu.roll(wet_all, shift, axis)))
        for shift, axis in turns
    ]
    diagonal = 0.5 * mask_all + ((weights[0] + weights[1]) + (weights[2] + weights[3]))
    found = []
    for begin in (start_all, mask_all):
        residual = direction = begin
        answer = jnp.zeros_like(begin)
        for turn in range(iters):
            answer = answer + alpha_ref[turn] * direction
            if turn + 1 < iters:
                applied = diagonal * direction
                for weight, (shift, axis) in zip(weights, turns):
                    applied = applied - weight * pltpu.roll(direction, shift, axis)
                residual = residual - alpha_ref[turn] * applied
                direction = residual + beta_ref[turn] * direction
        found.append(answer[HALF : HALF + rows, 0:cols])

    def forward(first, count):
        lhs = jnp.concatenate(
            [
                xs[c, first + a : first + a + count].reshape(count * cols, chan)
                for a in range(3)
                for c in range(3)
            ],
            axis=1,
        )
        return jnp.dot(lhs, w_ref[...], preferred_element_type=F32) + bias_ref[...]

    for step in range(1, group):
        spot, place = peer(step)
        remote(mean_buf.at[spot], mean_buf.at[spot], mean_send.at[step - 1], mean_recv.at[spot], place).wait_recv()
    total = jnp.sum(mean_buf[...], axis=0)
    mean = jnp.sum(total[1:2, :], axis=1, keepdims=True) / jnp.sum(total[0:1, :], axis=1, keepdims=True)
    forcing = mask * (found[0] - mean * found[1])
    columns = forcing.T

    block = 4
    bias_sum = jnp.zeros((HALF, chan), F32)
    proj_sum = jnp.zeros((HALF, chan), F32)
    for first in range(0, rows, block):
        preact = forward(first, block)
        for at in range(block):
            row = first + at
            pre = preact[at * cols : (at + 1) * cols]
            sigma = jax.nn.sigmoid(pre)
            force = jnp.broadcast_to(columns[:, row : row + 1], (cols, chan))
            active = pre * sigma
            cotangent = (force * proj_ref[...] * (sigma * (1.0 + pre * (1.0 - sigma)))).astype(BF16)
            gs[1, row + 1] = cotangent
            wide = cotangent.astype(F32)
            gbuf[0, row : row + 1, :] = wide[0:1]
            gbuf[1, row : row + 1, :] = wide[cols - 1 : cols]
            bias_sum = bias_sum + jnp.sum(wide.reshape(cols // HALF, HALF, chan), axis=0)
            proj_sum = proj_sum + jnp.sum((active * force).reshape(cols // HALF, HALF, chan), axis=0)
    small_buf[me] = jnp.concatenate(
        [jnp.sum(bias_sum, axis=0, keepdims=True), jnp.sum(proj_sum, axis=0, keepdims=True)], axis=0
    )

    g_copies = halo_copies(
        g_send,
        g_recv,
        (gs.at[1, 1], gs.at[1, rows + 1], gs.at[1, rows], gs.at[1, 0]),
        None,
        ((gbuf.at[0], gl_in.at[0]), (gbuf.at[1], gl_in.at[1])),
        (
            (gbuf.at[0, 0:HALF], gc_in.at[0]),
            (gbuf.at[1, 0:HALF], gc_in.at[1]),
            (gbuf.at[0, rows - HALF : rows], gc_in.at[2]),
            (gbuf.at[1, rows - HALF : rows], gc_in.at[3]),
        ),
    )
    for at in (4, 5, 6, 7, 2, 3, 0, 1):
        guarded(g_copies[at][0], g_copies[at][2].start)
    small_copies = []
    for step in range(1, group):
        spot, place = peer(step)
        small_copies.append(remote(small_buf.at[me], small_buf.at[me], small_send.at[step - 1], small_recv.at[me], place))
        small_copies[-1].start()
    clear(has_s, (gs.at[1, rows + 1], gc_in.at[0], gc_in.at[1]))
    clear(has_n, (gs.at[1, 0], gc_in.at[2], gc_in.at[3]))

    right = gs[1, 1 : rows + 1].reshape(rows * cols, chan)
    pairs = nlat // 2
    own_lat = chan // nlat
    parity, half_at = lax.rem(la, 2), la // 2
    sends = []
    for a in range(3):
        for c in range(3):
            left = xs[c, a : a + rows].reshape(rows * cols, chan)
            part = lax.dot_general(left, right, (((0,), (0,)), ((), ())), preferred_element_type=F32)
            if fast:
                for lat_at in range(nlat):
                    g1[lat_at, 3 * a + c] = part[lat_at * own_lat : (lat_at + 1) * own_lat].astype(BF16)
            else:
                gw_ref[3 * a + c] = part
        if fast:
            for pair in range(pairs):
                sends.append(
                    remote(
                        g1.at[2 * pair + 1 - parity, 3 * a : 3 * a + 3],
                        r1.at[pair, 3 * a : 3 * a + 3],
                        r1_send.at[3 * pair + a],
                        r1_recv.at[3 * pair + a],
                        {"lat": la + 1 - 2 * parity},
                    )
                )
                sends[-1].start()
    first_stage = list(sends)

    for row in range(rows):
        wide = gs[1, row + 1].astype(F32)
        gs[0, row + 1] = pltpu.roll(wide, 1, 0).astype(BF16)
        gs[2, row + 1] = pltpu.roll(wide, cols - 1, 0).astype(BF16)

    second_stage = []
    if fast:
        for copy in first_stage:
            copy.wait_recv()
        for step in range(1, pairs):
            other = lax.rem(half_at + step, pairs)
            s1[step] = (g1[2 * other + parity].astype(F32) + r1[other].astype(F32)).astype(BF16)
            second_stage.append(
                remote(s1.at[step], r2.at[step], r2_send.at[step], r2_recv.at[step], {"lat": 2 * other + parity})
            )
            second_stage[-1].start()

    for at in range(8):
        guarded(g_copies[at][1], g_copies[at][2].wait_recv)
    fix_ends(
        gs,
        (gc_in[3, last : last + 1, :], gc_in[2, last : last + 1, :]),
        (gc_in[1, 0:1, :], gc_in[0, 0:1, :]),
    )
    for row in range(rows):
        fix(gs, row + 1, gl_in[1, row : row + 1, :], gl_in[0, row : row + 1, :])

    def backward(first, count):
        lhs = jnp.concatenate(
            [
                gs[c, first + a : first + a + count].reshape(count * cols, chan)
                for a in range(3)
                for c in range(3)
            ],
            axis=1,
        )
        result = jnp.dot(lhs, wb[...], preferred_element_type=F32).astype(BF16)
        gh_ref[0, first : first + count] = result.reshape(count, cols, chan)

    for step in range(1, group):
        spot, place = peer(step)
        remote(small_buf.at[spot], small_buf.at[spot], small_send.at[step - 1], small_recv.at[spot], place).wait_recv()
    small_dp[dp] = jnp.sum(small_buf[...], axis=0)
    small_dp_copies = []
    for step in range(1, ndp):
        place = {"dp": lax.rem(dp + step, ndp)}
        small_dp_copies.append(remote(small_dp.at[dp], small_dp.at[dp], sdp_send.at[step - 1], sdp_recv.at[dp], place))
        small_dp_copies[-1].start()

    quarter = rows // 4
    backward(0, quarter)
    third_stage, fourth_stage = [], []
    if fast:
        share = own_lat // nlon
        lat_sum = g1[2 * half_at + parity].astype(F32) + r1[half_at].astype(F32)
        for copy in second_stage:
            copy.wait_recv()
        for step in range(1, pairs):
            lat_sum = lat_sum + r2[step].astype(F32)
        for lon_at in range(nlon):
            b3[lon_at] = jnp.concatenate(
                [lat_sum[tap, lon_at * share : (lon_at + 1) * share] for tap in range(9)], axis=0
            ).astype(BF16)
        for step in range(1, nlon):
            other = lax.rem(lo + step, nlon)
            third_stage.append(remote(b3.at[other], r3.at[step], r3_send.at[step], r3_recv.at[step], {"lon": other}))
            third_stage[-1].start()
    backward(quarter, quarter)
    backward(2 * quarter, quarter)
    if fast:
        for copy in third_stage:
            copy.wait_recv()
        lon_sum = b3[lo].astype(F32)
        for step in range(1, nlon):
            lon_sum = lon_sum + r3[step].astype(F32)
        s4[dp] = lon_sum.astype(BF16)
        for step in range(1, ndp):
            place = {"dp": lax.rem(dp + step, ndp)}
            fourth_stage.append(remote(s4.at[dp], s4.at[dp], r4_send.at[step - 1], r4_recv.at[dp], place))
            fourth_stage[-1].start()
    backward(3 * quarter, quarter)

    cells = ndp * nlat * nlon * rows * cols
    scale = 1.0 / math.sqrt(cells)
    for step in range(1, ndp):
        other = lax.rem(dp + step, ndp)
        remote(small_dp.at[other], small_dp.at[other], sdp_send.at[step - 1], sdp_recv.at[other], {"dp": other}).wait_recv()
        if fast:
            remote(s4.at[other], s4.at[other], r4_send.at[step - 1], r4_recv.at[other], {"dp": other}).wait_recv()
    if fast:
        gw_ref[...] = jnp.sum(s4[...].astype(F32), axis=0) * scale
    sum_ref[...] = jnp.sum(small_dp[...], axis=0) * scale

    for guard, _, copy in x_copies + g_copies:
        guarded(guard, copy.wait_send)
    for copy in mean_copies + small_copies + small_dp_copies + first_stage + second_stage + third_stage + fourth_stage:
        copy.wait_send()


def shards(hidden_in, conv_weight, conv_bias, proj_weight, ocean_depth, sea_mask, step_alpha, step_beta, surface_cotangent):
    _, rows, cols, chan = hidden_in.shape
    ndp, nlat, nlon = (lax.axis_size(axis) for axis in ("dp", "lat", "lon"))
    group = nlat * nlon
    own_lat = chan // nlat
    share = own_lat // nlon
    fast = nlat % 2 == 0 and own_lat % 16 == 0 and share % 8 == 0
    iters = step_alpha.shape[0]
    dims = (ndp, nlat, nlon, rows, cols, chan, iters, fast)
    dma = lambda count: pltpu.SemaphoreType.DMA((max(count, 1),))
    scratch = [
        pltpu.VMEM((3, rows + 2, cols, chan), BF16),
        pltpu.VMEM((3, rows + 2, cols, chan), BF16),
        pltpu.VMEM((9 * chan, chan), BF16),
        pltpu.VMEM((2, rows, cols), F32),
        pltpu.VMEM((2, 2, HALF, cols), F32),
        pltpu.VMEM((3, rows, chan), F32),
        pltpu.VMEM((2, 2, rows, chan), F32),
        pltpu.VMEM((4, 2, HALF, chan), F32),
        pltpu.VMEM((2, rows, chan), F32),
        pltpu.VMEM((2, rows, chan), F32),
        pltpu.VMEM((4, HALF, chan), F32),
        pltpu.VMEM((group, 2, cols), F32),
        pltpu.VMEM((group, 2, chan), F32),
        pltpu.VMEM((ndp, 2, chan), F32),
        dma(10), dma(10), dma(8), dma(8),
        dma(group), dma(group), dma(group), dma(group), dma(ndp), dma(ndp),
    ]
    if fast:
        pairs = nlat // 2
        scratch += [
            pltpu.VMEM((nlat, 9, own_lat, chan), BF16),
            pltpu.VMEM((pairs, 9, own_lat, chan), BF16),
            pltpu.VMEM((pairs, 9, own_lat, chan), BF16),
            pltpu.VMEM((pairs, 9, own_lat, chan), BF16),
            pltpu.VMEM((nlon, 9 * share, chan), BF16),
            pltpu.VMEM((nlon, 9 * share, chan), BF16),
            pltpu.VMEM((ndp, 9 * share, chan), BF16),
            dma(3 * pairs), dma(3 * pairs), dma(pairs), dma(pairs), dma(nlon), dma(nlon), dma(ndp), dma(ndp),
        ]
    vmem, smem = pl.BlockSpec(memory_space=pltpu.VMEM), pl.BlockSpec(memory_space=pltpu.SMEM)
    gw_shape = (9 * share, chan) if fast else (9, chan, chan)
    grad_hidden, weight_part, sums = pl.pallas_call(
        functools.partial(kernel, dims),
        out_shape=(
            jax.ShapeDtypeStruct(hidden_in.shape, BF16),
            jax.ShapeDtypeStruct(gw_shape, F32),
            jax.ShapeDtypeStruct((2, chan), F32),
        ),
        in_specs=[vmem] * 6 + [smem] * 2 + [vmem],
        out_specs=(vmem, vmem, vmem),
        scratch_shapes=scratch,
        compiler_params=pltpu.CompilerParams(collective_id=0, has_side_effects=True, vmem_limit_bytes=48 * 1024 * 1024),
    )(
        hidden_in,
        conv_weight.reshape(9 * chan, chan),
        conv_bias.reshape(1, chan),
        proj_weight.reshape(1, chan),
        ocean_depth,
        sea_mask,
        step_alpha,
        step_beta,
        surface_cotangent,
    )
    if fast:
        grad_weight = weight_part.reshape(3, 3, share, chan).transpose(2, 0, 1, 3)
    else:
        blocks = weight_part.reshape(3, 3, chan, chan).transpose(2, 0, 1, 3)
        spatial = lax.psum_scatter(blocks, ("lat", "lon"), scatter_dimension=0, tiled=True)
        grad_weight = lax.psum(spatial, "dp") * (1.0 / math.sqrt(ndp * group * rows * cols))
    return grad_hidden, grad_weight, sums[0], sums[1]


def solution(mesh):
    in_specs = (
        P("dp", "lat", "lon", None),
        P(),
        P(),
        P(),
        P("lat", "lon"),
        P("lat", "lon"),
        P(),
        P(),
        P("dp", "lat", "lon"),
    )
    out_specs = (P("dp", "lat", "lon", None), P(("lat", "lon"), None, None, None), P(), P())
    return jax.shard_map(shards, mesh=mesh, in_specs=in_specs, out_specs=out_specs, check_vma=False)
```

```python
import functools
import math

import jax
import jax.numpy as jnp
from jax import lax
from jax.experimental import pallas as pl
from jax.experimental.pallas import tpu as pltpu
from jax.sharding import PartitionSpec as P

MESH = pl.DeviceIdType.MESH
F32 = jnp.float32
BF16 = jnp.bfloat16
HALF = 8


def remote(src, dst, send, recv, device):
    return pltpu.make_async_remote_copy(
        src_ref=src, dst_ref=dst, send_sem=send, recv_sem=recv, device_id=device, device_id_type=MESH
    )


def kernel(dims, *refs):
    ndp, nlat, nlon, rows, cols, chan, iters, fast = dims
    (x_hbm, w_hbm, bias_ref, proj_ref, depth_hbm, mask_hbm, alpha_ref, beta_ref, ct_hbm) = refs[:9]
    gh_ref, gw_ref, sum_ref = refs[9:12]
    (xs, gs, wb, fld, q_in, ebuf, el_in, ec_in, gbuf, gl_in, gc_in, mean_buf, small_buf, small_dp) = refs[12:26]
    (x_send, x_recv, g_send, g_recv, mean_send, mean_recv, small_send, small_recv, sdp_send, sdp_recv) = refs[26:36]
    (x_ref, w_ref, depth_ref, mask_ref, ct_ref, load_sem, pre_buf) = refs[36:43]
    if fast:
        (g1, r1, s1, r2, b3, r3, s4) = refs[43:50]
        (r1_send, r1_recv, r2_send, r2_recv, r3_send, r3_recv, r4_send, r4_recv) = refs[50:58]
    dp, la, lo = lax.axis_index("dp"), lax.axis_index("lat"), lax.axis_index("lon")
    group = nlat * nlon
    me = la * nlon + lo
    west, east = lax.rem(lo + nlon - 1, nlon), lax.rem(lo + 1, nlon)
    has_n, has_s = la > 0, la < nlat - 1

    def peer(step):
        spot = lax.rem(me + step, group)
        return spot, {"lat": spot // nlon, "lon": lax.rem(spot, nlon)}

    held = ((mask_hbm, mask_ref), (depth_hbm, depth_ref), (ct_hbm, ct_ref), (x_hbm, x_ref), (w_hbm, w_ref))
    loads = [pltpu.make_async_copy(hbm, ref, load_sem.at[at]) for at, (hbm, ref) in enumerate(held)]
    for load in loads:
        load.start()

    barrier = pltpu.get_barrier_semaphore()
    for step in range(1, group):
        pl.semaphore_signal(barrier, inc=1, device_id=peer(step)[1], device_id_type=MESH)
    for step in range(1, ndp):
        pl.semaphore_signal(barrier, inc=1, device_id={"dp": lax.rem(dp + step, ndp)}, device_id_type=MESH)

    for load in loads[:3]:
        load.wait()
    mask = mask_ref[...].astype(F32)
    wet = mask * depth_ref[...]
    start = mask * ct_ref[0]
    fld[0] = wet
    fld[1] = start
    lane = lax.broadcasted_iota(jnp.int32, (rows, cols), 1)
    ebuf[1] = jnp.where(
        lane < 16,
        wet,
        jnp.where(lane < 64, pltpu.roll(start, 16, 1), jnp.where(lane < cols - 16, pltpu.roll(start, cols - 16, 1), wet)),
    )
    mean_buf[me] = jnp.concatenate(
        [jnp.sum(mask, axis=0, keepdims=True), jnp.sum(start, axis=0, keepdims=True)], axis=0
    )
    loads[3].wait()
    for row in range(rows):
        ebuf[0, row : row + 1, :] = x_ref[0, row, 0:16, :].astype(F32)[0:1]
        ebuf[2, row : row + 1, :] = x_ref[0, row, cols - 16 : cols, :].astype(F32)[15:16]

    pl.semaphore_wait(barrier, group - 1 + ndp - 1)

    def halo_copies(send, recv, row_pair, q_pair, line_pair, corner):
        north, south = {"lat": la - 1}, {"lat": la + 1}
        out = []
        out.append((has_n, has_s, remote(row_pair[0], row_pair[1], send.at[0], recv.at[0], north)))
        out.append((has_s, has_n, remote(row_pair[2], row_pair[3], send.at[1], recv.at[1], south)))
        for at in range(2):
            out.append((None, None, remote(line_pair[at][0], line_pair[at][1], send.at[2 + at], recv.at[2 + at], {"lon": (west, east)[at]})))
        for at in range(4):
            up = at < 2
            place = {"lat": la - 1 if up else la + 1, "lon": (west, east)[at % 2]}
            guards = (has_n, has_s) if up else (has_s, has_n)
            out.append(guards + (remote(corner[at][0], corner[at][1], send.at[4 + at], recv.at[4 + at], place),))
        if q_pair is not None:
            out.append((has_n, has_s, remote(q_pair[0], q_pair[1], send.at[8], recv.at[8], north)))
            out.append((has_s, has_n, remote(q_pair[2], q_pair[3], send.at[9], recv.at[9], south)))
        return out

    def guarded(guard, action):
        if guard is None:
            action()
        else:
            pl.when(guard)(action)

    def clear(guard, views):
        @pl.when(jnp.logical_not(guard))
        def _():
            for view in views:
                view[...] = jnp.zeros(view.shape, view.dtype)

    x_copies = halo_copies(
        x_send,
        x_recv,
        (x_ref.at[0, 0], xs.at[1, rows + 1], x_ref.at[0, rows - 1], xs.at[1, 0]),
        (fld.at[:, 0:HALF], q_in.at[0], fld.at[:, rows - HALF : rows], q_in.at[1]),
        ((ebuf.at[0:2], el_in.at[0]), (ebuf.at[1:3], el_in.at[1])),
        (
            (ebuf.at[0:2, 0:HALF], ec_in.at[0]),
            (ebuf.at[1:3, 0:HALF], ec_in.at[1]),
            (ebuf.at[0:2, rows - HALF : rows], ec_in.at[2]),
            (ebuf.at[1:3, rows - HALF : rows], ec_in.at[3]),
        ),
    )
    mean_copies = []
    for step in range(1, group):
        spot, place = peer(step)
        mean_copies.append(remote(mean_buf.at[me], mean_buf.at[me], mean_send.at[step - 1], mean_recv.at[me], place))
        mean_copies[-1].start()
    for at in (8, 9, 4, 5, 6, 7, 2, 3, 0, 1):
        guarded(x_copies[at][0], x_copies[at][2].start)
    clear(has_s, (xs.at[1, rows + 1], q_in.at[0], ec_in.at[0], ec_in.at[1]))
    clear(has_n, (xs.at[1, 0], q_in.at[1], ec_in.at[2], ec_in.at[3]))

    loads[4].wait()
    for tap in range(9):
        wb[tap * chan : (tap + 1) * chan, :] = w_ref[(8 - tap) * chan : (9 - tap) * chan, :].astype(F32).T.astype(BF16)
    for row in range(rows):
        own = x_ref[0, row]
        wide = own.astype(F32)
        xs[1, row + 1] = own
        xs[0, row + 1] = pltpu.roll(wide, 1, 0).astype(BF16)
        xs[2, row + 1] = pltpu.roll(wide, cols - 1, 0).astype(BF16)

    for at in range(10):
        guarded(x_copies[at][1], x_copies[at][2].wait_recv)

    tile_row = lax.broadcasted_iota(jnp.int32, (16, chan), 0)

    def fix(stack, row, left, right):
        head = stack[0, row, 0:16, :].astype(F32)
        stack[0, row, 0:16, :] = jnp.where(tile_row == 0, left, head).astype(BF16)
        tail = stack[2, row, cols - 16 : cols, :].astype(F32)
        stack[2, row, cols - 16 : cols, :] = jnp.where(tile_row == 15, right, tail).astype(BF16)

    def fix_ends(stack, top, bottom):
        for row, (left, right) in ((0, top), (rows + 1, bottom)):
            wide = stack[1, row].astype(F32)
            stack[0, row] = pltpu.roll(wide, 1, 0).astype(BF16)
            stack[2, row] = pltpu.roll(wide, cols - 1, 0).astype(BF16)
            fix(stack, row, left, right)

    last = HALF - 1
    fix_ends(
        xs,
        (ec_in[3, 1, last : last + 1, :], ec_in[2, 0, last : last + 1, :]),
        (ec_in[1, 1, 0:1, :], ec_in[0, 0, 0:1, :]),
    )
    for row in range(rows):
        fix(xs, row + 1, el_in[1, 1, row : row + 1, :], el_in[0, 0, row : row + 1, :])

    def forward(first, count):
        lhs = jnp.concatenate(
            [
                xs[c, first + a : first + a + count].reshape(count * cols, chan)
                for a in range(3)
                for c in range(3)
            ],
            axis=1,
        )
        return jnp.dot(lhs, w_ref[...], preferred_element_type=F32) + bias_ref[...]

    block = 4
    for first in range(0, rows, block):
        pre_buf[first * cols : (first + block) * cols, :] = forward(first, block)

    tall = rows + 2 * HALF
    side_lane = lax.broadcasted_iota(jnp.int32, (tall, cols), 1)
    from_west = jnp.concatenate([ec_in[3, 0], el_in[1, 0], ec_in[1, 0]], axis=0)
    from_east = jnp.concatenate([ec_in[2, 1], el_in[0, 1], ec_in[0, 1]], axis=0)
    near = jnp.logical_or(side_lane < iters - 1, side_lane >= cols - (iters - 1))
    wet_side = jnp.where(near, jnp.where(side_lane < 64, from_east, from_west), 0.0)
    start_side = jnp.where(
        near, jnp.where(side_lane < 64, pltpu.roll(from_east, cols - 16, 1), pltpu.roll(from_west, 16, 1)), 0.0
    )
    wet_all = jnp.concatenate([jnp.concatenate([q_in[1, 0], fld[0], q_in[0, 0]], axis=0), wet_side], axis=1)
    start_all = jnp.concatenate([jnp.concatenate([q_in[1, 1], fld[1], q_in[0, 1]], axis=0), start_side], axis=1)
    turns = ((1, 0), (tall - 1, 0), (1, 1), (2 * cols - 1, 1))
    mask_all = jnp.where(wet_all > 0.0, 1.0, 0.0)
    weights = [
        mask_all * pltpu.roll(mask_all, shift, axis) * (0.5 * (wet_all + pltpu.roll(wet_all, shift, axis)))
        for shift, axis in turns
    ]
    diagonal = 0.5 * mask_all + ((weights[0] + weights[1]) + (weights[2] + weights[3]))
    found = []
    for begin in (start_all, mask_all):
        residual = direction = begin
        answer = jnp.zeros_like(begin)
        for turn in range(iters):
            answer = answer + alpha_ref[turn] * direction
            if turn + 1 < iters:
                applied = diagonal * direction
                for weight, (shift, axis) in zip(weights, turns):
                    applied = applied - weight * pltpu.roll(direction, shift, axis)
                residual = residual - alpha_ref[turn] * applied
                direction = residual + beta_ref[turn] * direction
        found.append(answer[HALF : HALF + rows, 0:cols])

    for step in range(1, group):
        spot, place = peer(step)
        remote(mean_buf.at[spot], mean_buf.at[spot], mean_send.at[step - 1], mean_recv.at[spot], place).wait_recv()
    total = jnp.sum(mean_buf[...], axis=0)
    mean = jnp.sum(total[1:2, :], axis=1, keepdims=True) / jnp.sum(total[0:1, :], axis=1, keepdims=True)
    forcing = mask * (found[0] - mean * found[1])
    columns = forcing.T

    bias_sum = jnp.zeros((HALF, chan), F32)
    proj_sum = jnp.zeros((HALF, chan), F32)
    for first in range(0, rows, block):
        for at in range(block):
            row = first + at
            pre = pre_buf[row * cols : (row + 1) * cols, :]
            sigma = jax.nn.sigmoid(pre)
            force = jnp.broadcast_to(columns[:, row : row + 1], (cols, chan))
            active = pre * sigma
            cotangent = (force * proj_ref[...] * (sigma * (1.0 + pre * (1.0 - sigma)))).astype(BF16)
            gs[1, row + 1] = cotangent
            wide = cotangent.astype(F32)
            gbuf[0, row : row + 1, :] = wide[0:1]
            gbuf[1, row : row + 1, :] = wide[cols - 1 : cols]
            bias_sum = bias_sum + jnp.sum(wide.reshape(cols // HALF, HALF, chan), axis=0)
            proj_sum = proj_sum + jnp.sum((active * force).reshape(cols // HALF, HALF, chan), axis=0)
    small_buf[me] = jnp.concatenate(
        [jnp.sum(bias_sum, axis=0, keepdims=True), jnp.sum(proj_sum, axis=0, keepdims=True)], axis=0
    )

    g_copies = halo_copies(
        g_send,
        g_recv,
        (gs.at[1, 1], gs.at[1, rows + 1], gs.at[1, rows], gs.at[1, 0]),
        None,
        ((gbuf.at[0], gl_in.at[0]), (gbuf.at[1], gl_in.at[1])),
        (
            (gbuf.at[0, 0:HALF], gc_in.at[0]),
            (gbuf.at[1, 0:HALF], gc_in.at[1]),
            (gbuf.at[0, rows - HALF : rows], gc_in.at[2]),
            (gbuf.at[1, rows - HALF : rows], gc_in.at[3]),
        ),
    )
    for at in (4, 5, 6, 7, 2, 3, 0, 1):
        guarded(g_copies[at][0], g_copies[at][2].start)
    small_copies = []
    for step in range(1, group):
        spot, place = peer(step)
        small_copies.append(remote(small_buf.at[me], small_buf.at[me], small_send.at[step - 1], small_recv.at[me], place))
        small_copies[-1].start()
    clear(has_s, (gs.at[1, rows + 1], gc_in.at[0], gc_in.at[1]))
    clear(has_n, (gs.at[1, 0], gc_in.at[2], gc_in.at[3]))

    right = gs[1, 1 : rows + 1].reshape(rows * cols, chan)
    pairs = nlat // 2
    own_lat = chan // nlat
    parity, half_at = lax.rem(la, 2), la // 2
    sends = []
    for a in range(3):
        for c in range(3):
            left = xs[c, a : a + rows].reshape(rows * cols, chan)
            part = lax.dot_general(left, right, (((0,), (0,)), ((), ())), preferred_element_type=F32)
            if fast:
                for lat_at in range(nlat):
                    g1[lat_at, 3 * a + c] = part[lat_at * own_lat : (lat_at + 1) * own_lat].astype(BF16)
            else:
                gw_ref[3 * a + c] = part
        if fast:
            for pair in range(pairs):
                sends.append(
                    remote(
                        g1.at[2 * pair + 1 - parity, 3 * a : 3 * a + 3],
                        r1.at[pair, 3 * a : 3 * a + 3],
                        r1_send.at[3 * pair + a],
                        r1_recv.at[3 * pair + a],
                        {"lat": la + 1 - 2 * parity},
                    )
                )
                sends[-1].start()
    first_stage = list(sends)
    second_stage, third_stage, fourth_stage = [], [], []
    share = own_lat // nlon

    def run_second(a):
        taps = pl.ds(3 * a, 3)
        for pair in range(pairs):
            first_stage[a * pairs + pair].wait_recv()
        for step in range(1, pairs):
            other = lax.rem(half_at + step, pairs)
            s1[step, taps] = (g1[2 * other + parity, taps].astype(F32) + r1[other, taps].astype(F32)).astype(BF16)
            copy = remote(
                s1.at[step, taps],
                r2.at[step, taps],
                r2_send.at[3 * step + a],
                r2_recv.at[3 * step + a],
                {"lat": 2 * other + parity},
            )
            copy.start()
            second_stage.append(copy)

    def run_third(a):
        taps = pl.ds(3 * a, 3)
        for step in range(1, pairs):
            second_stage[a * (pairs - 1) + step - 1].wait_recv()
        lat_sum = g1[2 * half_at + parity, taps].astype(F32) + r1[half_at, taps].astype(F32)
        for step in range(1, pairs):
            lat_sum = lat_sum + r2[step, taps].astype(F32)
        for lon_at in range(nlon):
            b3[lon_at, a] = jnp.concatenate(
                [lat_sum[tap, lon_at * share : (lon_at + 1) * share] for tap in range(3)], axis=0
            ).astype(BF16)
        for step in range(1, nlon):
            other = lax.rem(lo + step, nlon)
            copy = remote(
                b3.at[other, a], r3.at[step, a], r3_send.at[3 * step + a], r3_recv.at[3 * step + a], {"lon": other}
            )
            copy.start()
            third_stage.append(copy)

    def run_fourth(a):
        for step in range(1, nlon):
            third_stage[a * (nlon - 1) + step - 1].wait_recv()
        lon_sum = b3[lo, a].astype(F32)
        for step in range(1, nlon):
            lon_sum = lon_sum + r3[step, a].astype(F32)
        s4[dp, a] = lon_sum.astype(BF16)
        for step in range(1, ndp):
            copy = remote(
                s4.at[dp, a],
                s4.at[dp, a],
                r4_send.at[3 * step - 3 + a],
                r4_recv.at[3 * dp + a],
                {"dp": lax.rem(dp + step, ndp)},
            )
            copy.start()
            fourth_stage.append(copy)

    if fast:
        for a in range(3):
            run_second(a)

    for row in range(rows):
        wide = gs[1, row + 1].astype(F32)
        gs[0, row + 1] = pltpu.roll(wide, 1, 0).astype(BF16)
        gs[2, row + 1] = pltpu.roll(wide, cols - 1, 0).astype(BF16)

    for at in range(8):
        guarded(g_copies[at][1], g_copies[at][2].wait_recv)
    fix_ends(
        gs,
        (gc_in[3, last : last + 1, :], gc_in[2, last : last + 1, :]),
        (gc_in[1, 0:1, :], gc_in[0, 0:1, :]),
    )
    for row in range(rows):
        fix(gs, row + 1, gl_in[1, row : row + 1, :], gl_in[0, row : row + 1, :])

    def backward(first, count):
        lhs = jnp.concatenate(
            [
                gs[c, first + a : first + a + count].reshape(count * cols, chan)
                for a in range(3)
                for c in range(3)
            ],
            axis=1,
        )
        result = jnp.dot(lhs, wb[...], preferred_element_type=F32).astype(BF16)
        gh_ref[0, first : first + count] = result.reshape(count, cols, chan)

    for step in range(1, group):
        spot, place = peer(step)
        remote(small_buf.at[spot], small_buf.at[spot], small_send.at[step - 1], small_recv.at[spot], place).wait_recv()
    small_dp[dp] = jnp.sum(small_buf[...], axis=0)
    small_dp_copies = []
    for step in range(1, ndp):
        place = {"dp": lax.rem(dp + step, ndp)}
        small_dp_copies.append(remote(small_dp.at[dp], small_dp.at[dp], sdp_send.at[step - 1], sdp_recv.at[dp], place))
        small_dp_copies[-1].start()

    quarter = rows // 4
    for a in range(3):
        if fast:
            run_third(a)
        if a < 1:
            backward(a * quarter, quarter)
    backward(quarter, quarter)
    backward(2 * quarter, quarter)
    if fast:
        for a in range(3):
            run_fourth(a)
    backward(3 * quarter, quarter)

    cells = ndp * nlat * nlon * rows * cols
    scale = 1.0 / math.sqrt(cells)
    for step in range(1, ndp):
        other = lax.rem(dp + step, ndp)
        remote(small_dp.at[other], small_dp.at[other], sdp_send.at[step - 1], sdp_recv.at[other], {"dp": other}).wait_recv()
        if fast:
            for a in range(3):
                remote(
                    s4.at[other, a], s4.at[other, a], r4_send.at[3 * step - 3 + a], r4_recv.at[3 * other + a], {"dp": other}
                ).wait_recv()
    if fast:
        for a in range(3):
            part = s4[0, a].astype(F32)
            for at in range(1, ndp):
                part = part + s4[at, a].astype(F32)
            gw_ref[3 * a * share : 3 * (a + 1) * share, :] = part * scale
    sum_ref[...] = jnp.sum(small_dp[...], axis=0) * scale

    for guard, _, copy in x_copies + g_copies:
        guarded(guard, copy.wait_send)
    for copy in mean_copies + small_copies + small_dp_copies + first_stage + second_stage + third_stage + fourth_stage:
        copy.wait_send()


def shards(hidden_in, conv_weight, conv_bias, proj_weight, ocean_depth, sea_mask, step_alpha, step_beta, surface_cotangent):
    _, rows, cols, chan = hidden_in.shape
    ndp, nlat, nlon = (lax.axis_size(axis) for axis in ("dp", "lat", "lon"))
    group = nlat * nlon
    own_lat = chan // nlat
    share = own_lat // nlon
    fast = nlat % 2 == 0 and own_lat % 16 == 0 and share % 8 == 0
    iters = step_alpha.shape[0]
    dims = (ndp, nlat, nlon, rows, cols, chan, iters, fast)
    dma = lambda count: pltpu.SemaphoreType.DMA((max(count, 1),))
    scratch = [
        pltpu.VMEM((3, rows + 2, cols, chan), BF16),
        pltpu.VMEM((3, rows + 2, cols, chan), BF16),
        pltpu.VMEM((9 * chan, chan), BF16),
        pltpu.VMEM((2, rows, cols), F32),
        pltpu.VMEM((2, 2, HALF, cols), F32),
        pltpu.VMEM((3, rows, chan), F32),
        pltpu.VMEM((2, 2, rows, chan), F32),
        pltpu.VMEM((4, 2, HALF, chan), F32),
        pltpu.VMEM((2, rows, chan), F32),
        pltpu.VMEM((2, rows, chan), F32),
        pltpu.VMEM((4, HALF, chan), F32),
        pltpu.VMEM((group, 2, cols), F32),
        pltpu.VMEM((group, 2, chan), F32),
        pltpu.VMEM((ndp, 2, chan), F32),
        dma(10), dma(10), dma(8), dma(8),
        dma(group), dma(group), dma(group), dma(group), dma(ndp), dma(ndp),
        pltpu.VMEM(hidden_in.shape, BF16),
        pltpu.VMEM((9 * chan, chan), BF16),
        pltpu.VMEM((rows, cols), F32),
        pltpu.VMEM((rows, cols), jnp.int32),
        pltpu.VMEM((1, rows, cols), F32),
        dma(5),
        pltpu.VMEM((rows * cols, chan), F32),
    ]
    if fast:
        pairs = nlat // 2
        scratch += [
            pltpu.VMEM((nlat, 9, own_lat, chan), BF16),
            pltpu.VMEM((pairs, 9, own_lat, chan), BF16),
            pltpu.VMEM((pairs, 9, own_lat, chan), BF16),
            pltpu.VMEM((pairs, 9, own_lat, chan), BF16),
            pltpu.VMEM((nlon, 3, 3 * share, chan), BF16),
            pltpu.VMEM((nlon, 3, 3 * share, chan), BF16),
            pltpu.VMEM((ndp, 3, 3 * share, chan), BF16),
            dma(3 * pairs), dma(3 * pairs), dma(3 * pairs), dma(3 * pairs), dma(3 * nlon), dma(3 * nlon), dma(3 * ndp), dma(3 * ndp),
        ]
    vmem, smem, hbm = (pl.BlockSpec(memory_space=space) for space in (pltpu.VMEM, pltpu.SMEM, pltpu.HBM))
    gw_shape = (9 * share, chan) if fast else (9, chan, chan)
    grad_hidden, weight_part, sums = pl.pallas_call(
        functools.partial(kernel, dims),
        out_shape=(
            pltpu.VMEM(hidden_in.shape, BF16),
            pltpu.VMEM(gw_shape, F32),
            pltpu.VMEM((2, chan), F32),
        ),
        in_specs=[hbm, hbm, vmem, vmem, hbm, hbm, smem, smem, hbm],
        out_specs=(vmem, vmem, vmem),
        scratch_shapes=scratch,
        compiler_params=pltpu.CompilerParams(collective_id=0, has_side_effects=True, vmem_limit_bytes=(66403328 if fast else 48 * 1024 * 1024)),
    )(
        hidden_in,
        conv_weight.reshape(9 * chan, chan),
        conv_bias.reshape(1, chan),
        proj_weight.reshape(1, chan),
        ocean_depth,
        sea_mask,
        step_alpha,
        step_beta,
        surface_cotangent,
    )
    if fast:
        grad_weight = weight_part.reshape(3, 3, share, chan).transpose(2, 0, 1, 3)
    else:
        blocks = weight_part.reshape(3, 3, chan, chan).transpose(2, 0, 1, 3)
        spatial = lax.psum_scatter(blocks, ("lat", "lon"), scatter_dimension=0, tiled=True)
        grad_weight = lax.psum(spatial, "dp") * (1.0 / math.sqrt(ndp * group * rows * cols))
    return grad_hidden, grad_weight, sums[0], sums[1]


def solution(mesh):
    in_specs = (
        P("dp", "lat", "lon", None),
        P(),
        P(),
        P(),
        P("lat", "lon"),
        P("lat", "lon"),
        P(),
        P(),
        P("dp", "lat", "lon"),
    )
    out_specs = (P("dp", "lat", "lon", None), P(("lat", "lon"), None, None, None), P(), P())
    return jax.shard_map(shards, mesh=mesh, in_specs=in_specs, out_specs=out_specs, check_vma=False)
```
